32 devices in a mesh: group: 4 (over y, x), dom: 8 (over z, core).
Axes of the slice: x: 2, y: 2, z: 4, core: 2. Of those that a mesh axis runs over, the one named last changes fastest.
Arguments:
- p_start: float32 [1024, 128], P(('group', 'dom')), may hold values from -60 to 60
- r_start: float32 [1024, 128], P(('group', 'dom')), may hold values from -60 to 60
- diag_shift: float32 [1024, 128], P(('group', 'dom')), may hold values from 0.5 to 2
- shifts: float32 [8], replicated, may hold values from 0.5 to 1.5
- block_values: float32 [1024, 6, 128, 128], P(('group', 'dom')), may hold values from -0.21875 to 0.21875
- block_cols: int32 [1024, 6], P(('group', 'dom')), may hold values from 0 to 95, as said below
- live_slots: int32 [1024], P(('group', 'dom')), may hold values from 2 to 6, as said below
- needed: int32 [32, 4, 16], P(('group', 'dom')), may hold values from 0 to 31
Outputs:
- basis: float32 [17, 1024, 128], P(None, ('group', 'dom'))
- gram: float32 [17, 17], replicated
The draws below stay inside these ranges and needn't reach their ends.
Inputs may be any that keep to these rules, and one draw needn't show every extreme that they name: `block_cols`: slot 0 of block row b is the row itself (b mod 32); a value below 32 names a block row of the same device, a value 32 + k * 16 + h names entry h of the device's list k of needed. Devices with dom index 0 never use list 0 in used slots, devices with the last dom index never list 1. Slots from live_slots on hold values in range but are not used. `live_slots`: the first block row of every device uses all 6 slots. needed[d, k] lists the local block rows that device d reads from its source s_k(d), in the order of its extended field.
All inputs are finite; a program needn't handle non-finite values.
Results may differ from the reference program's by a relative error of at most 0.0001.
Values sent between devices are 32-bit elements; how exact they have to be, the bound alone decides.
A program may use at most 64 MiB of HBM per device.

```python
import math
import jax
import jax.numpy as jnp
from jax import lax

BS = 128
S = 8
NB = 6
BR_DEV = 32
HALO = 16
NBLK = 1024
N_GROUP = 4
N_DOM = 8


def rough_vector(key):
    total = BR_DEV * N_GROUP * N_DOM
    owners = (jnp.arange(total) // BR_DEV).astype(jnp.float32)
    rise = jnp.exp(math.log(3.0) * owners / max(N_GROUP * N_DOM - 1, 1))
    cell = jnp.exp(jax.random.uniform(jax.random.fold_in(key, 1), (total, BS), jnp.float32, 0.0, math.log(10.0)))
    base = jax.random.normal(jax.random.fold_in(key, 2), (total, BS), jnp.float32)
    return base * cell * rise[:, None] * 0.25


def draw_p_start(key, part):
    return rough_vector(jax.random.fold_in(key, 101))


def draw_r_start(key, part):
    return rough_vector(jax.random.fold_in(key, 202))


def block_pattern(key):
    base_key = jax.random.fold_in(key, 303)
    total = BR_DEV * N_GROUP * N_DOM
    block_ids = jnp.arange(total, dtype=jnp.int32)
    dom_ids = block_ids // BR_DEV % N_DOM
    live = jax.random.randint(jax.random.fold_in(base_key, 1), (total,), 2, NB + 1)
    live = jnp.where(block_ids % BR_DEV == 0, NB, live).astype(jnp.int32)
    local_pick = jax.random.randint(jax.random.fold_in(base_key, 2), (total, NB), 0, BR_DEV)
    source_pick = jax.random.randint(jax.random.fold_in(base_key, 3), (total, NB), 0, 4)
    entry_pick = jax.random.randint(jax.random.fold_in(base_key, 4), (total, NB), 0, HALO)
    remote_pick = jax.random.randint(jax.random.fold_in(base_key, 5), (total, NB), 0, 2)
    missing = (source_pick == 0) & (dom_ids[:, None] == 0) | (source_pick == 1) & (dom_ids[:, None] == N_DOM - 1)
    remote = (remote_pick == 1) & jnp.logical_not(missing)
    cols = jnp.where(remote, BR_DEV + source_pick * HALO + entry_pick, local_pick)
    cols = cols.at[:, 0].set(block_ids % BR_DEV)
    return (cols.astype(jnp.int32), live)


def draw_block_cols(key, part):
    return block_pattern(key)[0]


def draw_live_slots(key, part):
    return block_pattern(key)[1]


def place_ends(values, stream_key, smallest, largest):
    longest = values.shape.index(max(values.shape))
    spots = []
    for shift in (0, 1):
        where = [jax.random.randint(jax.random.fold_in(stream_key, axis), (), 0, length) for axis, length in enumerate(values.shape)]
        where[longest] = (where[longest] + shift) % values.shape[longest]
        spots.append(tuple(where))
    return values.at[spots[0]].set(smallest).at[spots[1]].set(largest)


def shard_levels(own_key, extent, cuts, smallest, largest):
    def one(dim, parts):
        steps = jax.random.uniform(jax.random.fold_in(jax.random.fold_in(own_key, 6), dim), (parts,), jnp.float32, smallest / len(cuts), largest / len(cuts))
        return jnp.repeat(jnp.exp(steps), extent[dim] // parts).reshape((-1,) + (1,) * (len(extent) - dim - 1))

    level = one(*cuts[0])
    for cut in cuts[1:]:
        level = level * one(*cut)
    return level


def bell_draw(rng, shape, width, most, cuts=(), kind=jnp.bfloat16):
    array = jax.random.normal(rng, shape, jnp.float32) * width
    if len(cuts) > 0:
        array = shard_levels(rng, shape, cuts, -0.22, 0.18) * array
    return jnp.clip(array, min=-most, max=most).astype(kind)


def setup_inputs(seed: int = 0) -> dict:
    arg_keys = jax.random.split(jax.random.key(seed), 9)
    p_start = draw_p_start(jax.random.fold_in(arg_keys[8], 71), 0)
    r_start = draw_r_start(jax.random.fold_in(arg_keys[8], 71), 0)
    diag_shift = jnp.clip(jnp.exp(math.log(2.0) - 1.3862944 * jax.random.uniform(arg_keys[2], (NBLK, BS), jnp.float32) ** shard_levels(arg_keys[2], (NBLK, BS), ((0, 32),), -0.2, 0.2)), 0.5, 2.0)
    shifts = jnp.clip(jax.random.uniform(arg_keys[3], (S,), jnp.float32, 0.5, 1.5), 0.5, 1.5)
    block_values = bell_draw(arg_keys[4], (NBLK, NB, BS, BS), (NB * BS) ** -0.5, 0.21875, ((0, 32),), jnp.float32)
    block_cols = draw_block_cols(jax.random.fold_in(arg_keys[8], 71), 0)
    live_slots = draw_live_slots(jax.random.fold_in(arg_keys[8], 71), 0)
    needed = place_ends(jax.random.randint(arg_keys[7], (N_GROUP * N_DOM, 4, HALO), 0, BR_DEV), jax.random.fold_in(arg_keys[7], 1), 0, BR_DEV - 1).astype(jnp.int32)
    return dict(p_start=p_start, r_start=r_start, diag_shift=diag_shift, shifts=shifts, block_values=block_values, block_cols=block_cols, live_slots=live_slots, needed=needed)


def reference(p_start, r_start, diag_shift, shifts, block_values, block_cols, live_slots, needed):
    ndev = N_GROUP * N_DOM
    device_ids = jnp.arange(ndev, dtype=jnp.int32)
    group_ids = device_ids // N_DOM
    dom_ids = device_ids % N_DOM
    sources = [
        group_ids * N_DOM + jnp.maximum(dom_ids - 1, 0),
        group_ids * N_DOM + jnp.minimum(dom_ids + 1, N_DOM - 1),
        ((group_ids - 1) % N_GROUP) * N_DOM + dom_ids,
        ((group_ids + 1) % N_GROUP) * N_DOM + dom_ids,
    ]
    valid = [
        (dom_ids > 0).astype(jnp.float32),
        (dom_ids < N_DOM - 1).astype(jnp.float32),
        jnp.ones((ndev,), jnp.float32),
        jnp.ones((ndev,), jnp.float32),
    ]
    values = block_values.reshape(ndev, BR_DEV, NB, BS, BS)
    columns = block_cols.reshape(ndev, BR_DEV, NB)
    slot_ids = lax.broadcasted_iota(jnp.int32, (NBLK, NB), 1)
    masks = (slot_ids < live_slots[:, None]).astype(jnp.float32).reshape(ndev, BR_DEV, NB)

    def multiply(vector):
        blocks = vector.reshape(ndev, BR_DEV, BS)
        pieces = [blocks]
        for k in range(4):
            pieces.append(blocks[sources[k][:, None], needed[:, k, :]] * valid[k][:, None, None])
        extended = jnp.concatenate(pieces, axis=1)

        def single(item):
            vals, cols, live, ext = item
            picked = ext[cols] * live[:, :, None]
            return jnp.einsum("bsij,bsj->bi", vals, picked, precision=lax.Precision.HIGHEST)

        return lax.map(single, (values, columns, masks, extended)).reshape(NBLK, BS)

    def advance(vector, theta):
        return multiply(vector) + (diag_shift - theta) * vector

    p_fields = [p_start]
    for step in range(1, S + 1):
        p_fields.append(advance(p_fields[-1], shifts[step - 1]))
    r_fields = [r_start]
    for step in range(1, S):
        r_fields.append(advance(r_fields[-1], shifts[step - 1]))
    basis = jnp.stack(p_fields + r_fields)
    gram = jnp.einsum("kbi,lbi->kl", basis, basis, precision=lax.Precision.HIGHEST) / (NBLK * BS)
    return basis, gram
```

```python
import functools

import jax
import jax.numpy as jnp
from jax import lax
from jax.experimental import pallas as pl
from jax.experimental.pallas import tpu as pltpu
from jax.sharding import PartitionSpec as P

MESH = pl.DeviceIdType.MESH
SUB = 8
CHUNK_ROWS = 4


def split(x):
    hi = x.astype(jnp.bfloat16)
    lo = (x - hi.astype(jnp.float32)).astype(jnp.bfloat16)
    return hi, lo


def fold(tiles, lane):
    d = 1
    while len(tiles) > 1:
        low = (lane & d) == 0
        tiles = [
            jnp.where(low, u, v) + pltpu.roll(jnp.where(low, v, u), d, axis=1)
            for u, v in zip(tiles[0::2], tiles[1::2])
        ]
        d *= 2
    return tiles[0]


def kernel(n_group, n_dom, shifts, cols, live, needed, p0, r0, diag, a_hbm, basis, gram,
           a_v, xp0, xp1, xr0, xr1, f_v, idx, fields, g_own, g_all,
           a_sem, send_sem, recv_sem, g_send, g_recv):
    rows, slots, bs, _ = a_v.shape
    depth = shifts.shape[0]
    halo = needed.shape[1]
    chunks = a_sem.shape[0]
    per = rows // chunks
    tiles = bs // SUB
    zero_row = 5 * rows
    n = n_group * n_dom
    g, m = lax.axis_index("group"), lax.axis_index("dom")
    me = g * n_dom + m
    xs = ((xp0, xp1), (xr0, xr1))

    def chunk(c):
        part = pl.ds(c * per, per)
        return pltpu.make_async_copy(a_hbm.at[part], a_v.at[part], a_sem.at[c])

    for c in range(chunks):
        chunk(c).start()

    for field in xs:
        for ref in field:
            ref[pl.ds(rows, 2 * rows), :] = jnp.zeros((2 * rows, bs), jnp.float32)
            ref[pl.ds(zero_row, SUB), :] = jnp.zeros((SUB, bs), jnp.float32)
    xp0[pl.ds(0, rows), :] = p0[...]
    xr0[pl.ds(0, rows), :] = r0[...]

    barrier = pltpu.get_barrier_semaphore()

    def greet(d, carry):
        to = lax.rem(me + d, n)
        pl.semaphore_signal(barrier, inc=1, device_id=(to // n_dom, lax.rem(to, n_dom)), device_id_type=MESH)
        return carry

    lax.fori_loop(1, n, greet, 0)
    pl.semaphore_wait(barrier, n - 1)

    peers = (
        (g, lax.rem(m + 1, n_dom)),
        (g, lax.rem(m + n_dom - 1, n_dom)),
        (lax.rem(g + 1, n_group), m),
        (lax.rem(g + n_group - 1, n_group), m),
    )

    def copy(which, par, k):
        ref = xs[which][par]
        return pltpu.make_async_remote_copy(
            src_ref=ref.at[pl.ds(0, rows)],
            dst_ref=ref.at[pl.ds((1 + k) * rows, rows)],
            send_sem=send_sem.at[which, par, k],
            recv_sem=recv_sem.at[which, par, k],
            device_id=peers[k],
            device_id_type=MESH,
        )

    def guarded(ok, fn):
        if ok is None:
            fn()
        else:
            pl.when(ok)(fn)

    sends = (m < n_dom - 1, m > 0, None, None)
    recvs = (m > 0, m < n_dom - 1, None, None)
    order = (2, 3, 0, 1)

    def start(which, par):
        for k in order:
            guarded(sends[k], lambda k=k: copy(which, par, k).start())

    def wait_send(which, par):
        for k in order:
            guarded(sends[k], lambda k=k: copy(which, par, k).wait_send())

    def wait_recv(which, par):
        for k in order:
            guarded(recvs[k], lambda k=k: copy(which, par, k).wait_recv())

    start(0, 0)
    start(1, 0)

    def place(b, carry):
        for s in range(slots):
            c = cols[b, s]
            e = jnp.maximum(c - rows, 0)
            k = e // halo
            far = (1 + k) * rows + needed[k, lax.rem(e, halo)]
            at = jnp.where(c < rows, c, far)
            idx[b * slots + s] = jnp.where(s < live[b], at, zero_row)
        return carry

    lax.fori_loop(0, rows, place, 0)

    fields[...] = jnp.zeros_like(fields)
    basis[0] = p0[...]
    basis[depth + 1] = r0[...]
    fields[:, 0, :] = p0[...]
    fields[:, depth + 1, :] = r0[...]

    lane = lax.broadcasted_iota(jnp.int32, (SUB, bs), 1)
    l_id = lax.broadcasted_iota(jnp.int32, (2 * bs, bs), 0)
    c_id = lax.broadcasted_iota(jnp.int32, (2 * bs, bs), 1)
    spread = jnp.where(l_id % tiles == c_id // SUB, 1.0, 0.0).astype(jnp.bfloat16)
    z_row = lax.broadcasted_iota(jnp.int32, (rows * SUB, bs), 0)
    z_col = lax.broadcasted_iota(jnp.int32, (rows * SUB, bs), 1)
    z_keep = z_row % SUB == z_col % SUB

    def rows_of(which, par, lo, hi):
        x = xs[which][par]

        def body(b, carry):
            acc = [None] * tiles
            for s in range(slots):
                xv = jnp.broadcast_to(x[pl.ds(idx[b * slots + s], 1), :], (SUB, bs))
                for t in range(tiles):
                    term = a_v[b, s, pl.ds(t * SUB, SUB), :] * xv
                    acc[t] = term if s == 0 else acc[t] + term
            f_v[which, pl.ds(pl.multiple_of(b * SUB, SUB), SUB), :] = fold(acc, lane)
            return carry

        lax.fori_loop(lo, hi, body, 0)

    def finish(which, par, step):
        hi, lo = split(f_v[which])
        z = jnp.dot(jnp.concatenate([hi, lo], axis=1), spread, preferred_element_type=jnp.float32)
        y = jnp.where(z_keep, z, 0.0).reshape(rows, SUB, bs).sum(axis=1)
        return y + (diag[...] - shifts[step - 1]) * xs[which][par][pl.ds(0, rows), :]

    def emit(which, step, y):
        column = step if which == 0 else depth + 1 + step
        last = depth if which == 0 else depth - 1
        if step < last:
            xs[which][step % 2][pl.ds(0, rows), :] = y
            start(which, step % 2)
        basis[column] = y
        fields[:, column, :] = y

    for step in range(1, depth + 1):
        par = (step - 1) % 2
        chains = (0, 1) if step < depth else (0,)
        if step == 1:
            wait_recv(0, par)
            wait_recv(1, par)
            for c in range(chunks):
                chunk(c).wait()
                for which in chains:
                    rows_of(which, par, c * per, (c + 1) * per)
        for which in chains:
            if step > 1:
                wait_recv(which, par)
                rows_of(which, par, 0, rows)
            y = finish(which, par, step)
            if step > 1:
                wait_send(which, 1 - par)
            emit(which, step, y)
    wait_send(0, (depth - 1) % 2)
    wait_send(1, (depth - 2) % 2)

    def gram_row(b, acc):
        hi, lo = split(fields[b])
        both = jnp.concatenate([hi, lo], axis=0)
        return acc + lax.dot_general(
            both, both, (((1,), (1,)), ((), ())), preferred_element_type=jnp.float32
        )

    width = fields.shape[1]
    acc = lax.fori_loop(0, rows, gram_row, jnp.zeros((2 * width, 2 * width), jnp.float32))
    top = acc[:width] + acc[width:]
    part = top[:, :width] + top[:, width:]
    g_own[...] = jnp.concatenate([part, jnp.zeros((width, bs - width), jnp.float32)], axis=1)

    def share(d):
        to = lax.rem(me + d, n)
        return pltpu.make_async_remote_copy(
            src_ref=g_own,
            dst_ref=g_all.at[me],
            send_sem=g_send.at[d],
            recv_sem=g_recv.at[me],
            device_id=(to // n_dom, lax.rem(to, n_dom)),
            device_id_type=MESH,
        )

    def arrival(source):
        return pltpu.make_async_remote_copy(
            src_ref=g_own,
            dst_ref=g_all.at[source],
            send_sem=g_send.at[0],
            recv_sem=g_recv.at[source],
            device_id=(source // n_dom, lax.rem(source, n_dom)),
            device_id_type=MESH,
        )

    def send_one(d, carry):
        share(d).start()
        return carry

    def take_one(d, carry):
        arrival(lax.rem(me + d, n)).wait_recv()
        return carry

    def sent_one(d, carry):
        share(d).wait_send()
        return carry

    lax.fori_loop(1, n, send_one, 0)
    g_all[me] = g_own[...]
    lax.fori_loop(1, n, take_one, 0)
    lax.fori_loop(1, n, sent_one, 0)
    total = lax.fori_loop(1, n, lambda i, t: t + g_all[i], g_all[0])
    count = basis.shape[0]
    gram[...] = total[:count, :count] * (1.0 / (n * rows * bs))


def per_device(n_group, n_dom, p_start, r_start, diag_shift, shifts, block_values, block_cols, live_slots, needed):
    rows, bs = p_start.shape
    slots = block_values.shape[1]
    depth = shifts.shape[0]
    columns = 2 * depth + 1
    width = -(-columns // 16) * 16
    n = n_group * n_dom
    chunks = rows // CHUNK_ROWS
    smem = pl.BlockSpec(memory_space=pltpu.SMEM)
    vmem = pl.BlockSpec(memory_space=pltpu.VMEM)
    ext = pltpu.VMEM((5 * rows + SUB, bs), jnp.float32)
    return pl.pallas_call(
        functools.partial(kernel, n_group, n_dom),
        out_shape=(
            jax.ShapeDtypeStruct((columns, rows, bs), jnp.float32),
            jax.ShapeDtypeStruct((columns, columns), jnp.float32),
        ),
        in_specs=[smem, smem, smem, smem, vmem, vmem, vmem, pl.BlockSpec(memory_space=pl.ANY)],
        out_specs=(vmem, vmem),
        scratch_shapes=[
            pltpu.VMEM(block_values.shape, jnp.float32),
            ext, ext, ext, ext,
            pltpu.VMEM((2, rows * SUB, bs), jnp.float32),
            pltpu.SMEM((rows * slots,), jnp.int32),
            pltpu.VMEM((rows, width, bs), jnp.float32),
            pltpu.VMEM((width, bs), jnp.float32),
            pltpu.VMEM((n, width, bs), jnp.float32),
            pltpu.SemaphoreType.DMA((chunks,)),
            pltpu.SemaphoreType.DMA((2, 2, 4)),
            pltpu.SemaphoreType.DMA((2, 2, 4)),
            pltpu.SemaphoreType.DMA((n,)),
            pltpu.SemaphoreType.DMA((n,)),
        ],
        compiler_params=pltpu.CompilerParams(
            collective_id=0, has_side_effects=True, vmem_limit_bytes=60 * 1024 * 1024
        ),
    )(shifts, block_cols, live_slots, needed[0], p_start, r_start, diag_shift, block_values)


def solution(mesh):
    return jax.shard_map(
        functools.partial(per_device, mesh.shape["group"], mesh.shape["dom"]),
        mesh=mesh,
        in_specs=(
            P(("group", "dom"), None),
            P(("group", "dom"), None),
            P(("group", "dom"), None),
            P(),
            P(("group", "dom"), None, None, None),
            P(("group", "dom"), None),
            P(("group", "dom")),
            P(("group", "dom"), None, None),
        ),
        out_specs=(P(None, ("group", "dom"), None), P()),
        check_vma=False,
    )
```
